32 devices in a mesh: row: 4 (over x, core), col: 4 (over z), depth: 2 (over y).
Axes of the slice: x: 2, y: 2, z: 4, core: 2. Of those that a mesh axis runs over, the one named last changes fastest.
Arguments:
- acts: bfloat16 [256, 32768], P('depth', 'row'), may hold values from -6 to 6
- act_mask: int32 [256, 256], P('depth', 'row'), may hold values 0 or 1
- w1: bfloat16 [256, 32, 128, 128], P(('row', 'depth'), 'col'), may hold values from -0.09375 to 0.09375
- cols1: int32 [256, 32], P('row', 'col'), may hold values from 0 to 255, as said below
- bias1: float32 [32768], P('col'), may hold values from -3 to 3
- mask2: int32 [256, 256], P('depth', 'col'), may hold values 0 or 1
- w2: bfloat16 [256, 32, 128, 128], P(('col', 'depth'), 'row'), may hold values from -0.1875 to 0.1875
- cols2: int32 [256, 32], P('col', 'row'), may hold values from 0 to 255, as said below
- bias2: float32 [32768], P(('row', 'col')), may hold values from -3 to 3
Outputs:
- result: bfloat16 [256, 32768], P('depth', ('row', 'col'))
The draws below stay inside these ranges and needn't reach their ends.
Inputs may be any that keep to these rules, and one draw needn't show every extreme that they name: `cols1`: in each of the 256 block rows the 32 entries name different block columns, and for every g the entries g * 8 to g * 8 + 7 lie among block columns g * 64 to g * 64 + 63. `cols2`: in each of the 256 block rows the 32 entries name different block columns, and for every g the entries g * 8 to g * 8 + 7 lie among block columns g * 64 to g * 64 + 63.
All inputs are finite; a program needn't handle non-finite values. No bound on the sum of `act_mask` or of `mask2` on one device may be relied on, other than what follows from the above.
Results may differ from the reference program's by a relative error of at most 0.0047.
Values may be sent and summed in bfloat16 or wider, within the bound.
A program may use at most 128 MiB of HBM per device.

```python
import jax
import jax.numpy as jnp
from jax import lax

N = 32768
BS = 128
K = 32
NB = 256
NB_COL = 64
NB_ROW = 64
KC = 8
KR = 8
M = 256


def pattern(key, extent, per_group):
    groups = NB // extent
    score_values = jax.random.randint(key, (NB, groups, extent), 0, 1 << 20, dtype=jnp.int32)
    score_values = score_values * extent + jnp.arange(extent, dtype=jnp.int32)
    ranked = jnp.argsort(score_values, axis=-1)[:, :, :per_group].astype(jnp.int32)
    placed = ranked + (jnp.arange(groups, dtype=jnp.int32) * extent)[None, :, None]
    return placed.reshape(NB, groups * per_group).astype(jnp.int32)


def draw_cols1(key, part):
    return pattern(jax.random.fold_in(key, 1), NB_COL, KC)


def draw_cols2(key, part):
    return pattern(jax.random.fold_in(key, 2), NB_ROW, KR)


def with_ends(entries, own_key, smallest, high):
    index_at = [jax.random.randint(jax.random.fold_in(own_key, axis), (), 0, length) for axis, length in enumerate(entries.shape)]
    longest = entries.shape.index(max(entries.shape))
    neighbour = index_at[:longest] + [(index_at[longest] + 1) % entries.shape[longest]] + index_at[longest + 1:]
    return entries.at[tuple(index_at)].set(smallest).at[tuple(neighbour)].set(high)


def level_of(stream_key, shape, cuts, low, high):
    level = 1.0
    for position, blocks in cuts:
        draws = jax.random.uniform(jax.random.fold_in(jax.random.fold_in(stream_key, 6), position), (blocks,), jnp.float32, low / len(cuts), high / len(cuts))
        level = level * jnp.repeat(jnp.exp(draws), shape[position] // blocks).reshape((-1,) + (1,) * (len(shape) - 1 - position))
    return level


def normal_values(rng, shape, scale, most, pieces=(), kind=jnp.bfloat16):
    drawn = jax.random.normal(rng, shape, jnp.float32) * scale
    if len(pieces) > 0:
        drawn = level_of(rng, shape, pieces, -0.22, 0.18) * drawn
    return jnp.clip(drawn, min=-most, max=most).astype(kind)


def setup_inputs(seed: int = 0) -> dict:
    arg_keys = jax.random.split(jax.random.key(seed), 10)
    return {
        "acts": normal_values(arg_keys[0], (M, N), 1.0, 6.0, ((0, 2), (1, 4))),
        "act_mask": with_ends((jax.random.randint(arg_keys[1], (M, NB), 0, 4) < 3).astype(jnp.int32), jax.random.fold_in(arg_keys[1], 1), 0, 1),
        "w1": normal_values(arg_keys[2], (NB, K, BS, BS), (K * BS) ** -0.5, 0.09375, ((0, 8), (1, 4))),
        "cols1": draw_cols1(jax.random.fold_in(arg_keys[9], 71), 0),
        "bias1": normal_values(arg_keys[4], (N,), 0.5, 3.0, ((0, 4),), jnp.float32),
        "mask2": with_ends((jax.random.randint(arg_keys[5], (M, NB), 0, 4) < 3).astype(jnp.int32), jax.random.fold_in(arg_keys[5], 1), 0, 1),
        "w2": normal_values(arg_keys[6], (NB, K, BS, BS), (K * BS // 4) ** -0.5, 0.1875, ((0, 8), (1, 4))),
        "cols2": draw_cols2(jax.random.fold_in(arg_keys[9], 71), 0),
        "bias2": normal_values(arg_keys[8], (N,), 0.5, 3.0, ((0, 16),), jnp.float32),
    }


def dense_layer(inputs, weights, targets, bias):
    blocks_in = inputs.reshape(M, NB, BS).astype(jnp.float32)

    def advance(running_total, block_row):
        incoming_rows = blocks_in[:, block_row]
        tiles = weights[block_row].astype(jnp.float32)
        product = jnp.einsum("mb,kbc->mkc", incoming_rows, tiles)
        return running_total.at[:, targets[block_row]].add(product), None

    start_value = jnp.zeros((M, NB, BS), jnp.float32)
    summed, unused = lax.scan(advance, start_value, jnp.arange(NB, dtype=jnp.int32))
    return jnp.maximum(summed + bias.reshape(NB, BS), 0.0)


def reference(acts, act_mask, w1, cols1, bias1, mask2, w2, cols2, bias2):
    masked = acts.reshape(M, NB, BS) * act_mask[:, :, None].astype(jnp.bfloat16)
    masked = masked.reshape(M, N)
    first = dense_layer(masked, w1, cols1, bias1)
    hidden = (first * mask2[:, :, None].astype(jnp.float32)).astype(jnp.bfloat16)
    second = dense_layer(hidden.reshape(M, N), w2, cols2, bias2)
    return second.astype(jnp.bfloat16).reshape(M, N)
```

```python
import functools

import jax
import jax.numpy as jnp
from jax import lax
from jax.experimental import pallas as pl
from jax.experimental.pallas import tpu as pltpu
from jax.sharding import PartitionSpec as P


def fold_function(inputs, targets, stride):

    def add_tiles(running_total, tiles, first_row):

        def advance(number, total):
            offset = number * stride
            block_list = lax.dynamic_slice_in_dim(tiles, offset, stride, 0)
            incoming_rows = lax.dynamic_slice_in_dim(inputs, offset, stride, 1)
            wanted = lax.dynamic_slice_in_dim(targets, offset, stride, 0)
            product = jnp.einsum(
                "tws,wish->twih", incoming_rows, block_list, preferred_element_type=jnp.float32
            )
            flat_product = product.reshape(product.shape[0], -1, product.shape[-1])
            return total.at[:, wanted.reshape(-1)].add(flat_product)

        return lax.fori_loop(0, tiles.shape[0] // stride, advance, running_total)

    return add_tiles


def gathered_weights(acts, act_mask, w1, cols1, bias1, mask2, w2, cols2, bias2):
    block = w1.shape[-1]
    rows_dev = acts.shape[0]
    row_blocks = act_mask.shape[1]
    col_blocks = mask2.shape[1]
    row_index = lax.axis_index("row")
    col_index = lax.axis_index("col")
    masked = acts.reshape(rows_dev, row_blocks, block) * act_mask[:, :, None].astype(jnp.bfloat16)
    first_layer_destinations = cols1 - col_index * col_blocks
    second_targets = cols2 - row_index * row_blocks
    first_offset_value = jnp.zeros((rows_dev, col_blocks, block), jnp.float32)
    first_fold = fold_function(masked, first_layer_destinations, w1.shape[0])
    first_sum = first_fold(
        first_offset_value, lax.all_gather(w1, "depth", axis=0, tiled=True), jnp.int32(0)
    )
    bias_blocks = bias1.reshape(col_blocks, block)
    share = col_blocks // lax.axis_size("row")
    part_sum = lax.psum_scatter(first_sum, "row", scatter_dimension=1, tiled=True)
    bias_part = lax.dynamic_slice_in_dim(bias_blocks, row_index * share, share, 0)
    mask_part = lax.dynamic_slice_in_dim(mask2, row_index * share, share, 1)
    hidden_part = jnp.maximum(part_sum + bias_part, 0.0) * mask_part[:, :, None].astype(jnp.float32)
    hidden = lax.all_gather(hidden_part.astype(jnp.bfloat16), "row", axis=1, tiled=True)
    second_start = jnp.zeros((rows_dev, row_blocks, block), jnp.float32)
    second_fold = fold_function(hidden, second_targets, w2.shape[0])
    second_sum = second_fold(
        second_start, lax.all_gather(w2, "depth", axis=0, tiled=True), jnp.int32(0)
    )
    outcome = lax.psum_scatter(second_sum, "col", scatter_dimension=1, tiled=True)
    bias_out = bias2.reshape(outcome.shape[1], block)
    return jnp.maximum(outcome + bias_out, 0.0).astype(jnp.bfloat16).reshape(rows_dev, -1)


def sparse_kernel(per_step, entries, blocked, cols_ref, x_ref, w_ref, out_ref, total):
    step = pl.program_id(0)
    block = w_ref.shape[-1]

    @pl.when(step == 0)
    def _():
        total[...] = jnp.zeros_like(total)

    for row in range(per_step):
        if blocked:
            x = x_ref[row]
        else:
            x = x_ref[:, row * block:(row + 1) * block]
        for entry in range(0, entries, 2):
            pair = jnp.concatenate([w_ref[row, entry], w_ref[row, entry + 1]], axis=1)
            product = jnp.dot(x, pair, preferred_element_type=jnp.float32)
            base = (step * per_step + row) * entries + entry
            total[cols_ref[base]] += product[:, :block]
            total[cols_ref[base + 1]] += product[:, block:]

    @pl.when(step == pl.num_programs(0) - 1)
    def _():
        out_ref[...] = total[...].astype(out_ref.dtype)


def sparse_partial(x, weights, cols, out_blocks, blocked, kind=jnp.float32):
    stored, entries, block, _ = weights.shape
    rows = x.shape[1] if blocked else x.shape[0]
    per_step = 4 if stored % 4 == 0 else 1
    if blocked:
        x_spec = pl.BlockSpec((per_step, rows, block), lambda i, c: (i, 0, 0))
    else:
        x_spec = pl.BlockSpec((rows, per_step * block), lambda i, c: (0, i))
    return pl.pallas_call(
        functools.partial(sparse_kernel, per_step, entries, blocked),
        out_shape=jax.ShapeDtypeStruct((out_blocks, rows, block), kind),
        grid_spec=pltpu.PrefetchScalarGridSpec(
            num_scalar_prefetch=1,
            grid=(stored // per_step,),
            in_specs=[
                x_spec,
                pl.BlockSpec((per_step, entries, block, block), lambda i, c: (i, 0, 0, 0)),
            ],
            out_specs=pl.BlockSpec((out_blocks, rows, block), lambda i, c: (0, 0, 0)),
            scratch_shapes=[pltpu.VMEM((out_blocks, rows, block), jnp.float32)],
        ),
        compiler_params=pltpu.CompilerParams(
            dimension_semantics=("arbitrary",), vmem_limit_bytes=40 * 1024 * 1024
        ),
        cost_estimate=pl.CostEstimate(
            flops=2 * rows * weights.size, bytes_accessed=2 * weights.size, transcendentals=0
        ),
    )(cols.reshape(-1), x, weights)


def exchanged_rows(acts, act_mask, w1, cols1, bias1, mask2, w2, cols2, bias2):
    f32, bf16 = jnp.float32, jnp.bfloat16
    block = w1.shape[-1]
    stored1, stored2 = w1.shape[0], w2.shape[0]
    rows = acts.shape[0]
    row_blocks, col_blocks = act_mask.shape[1], mask2.shape[1]
    r, c, d = lax.axis_index("row"), lax.axis_index("col"), lax.axis_index("depth")
    n_row, n_col = lax.axis_size("row"), lax.axis_size("col")
    other = 1 - d
    swap = [(0, 1), (1, 0)]
    masked = (acts.reshape(rows, row_blocks, block) * act_mask[:, :, None].astype(bf16)).reshape(rows, -1)
    keep = lax.dynamic_slice_in_dim(masked, d * stored1 * block, stored1 * block, 1)
    give = lax.dynamic_slice_in_dim(masked, other * stored1 * block, stored1 * block, 1)
    taken = lax.ppermute(give, "depth", swap)
    to1 = lax.dynamic_slice_in_dim(cols1, d * stored1, stored1, 0) - c * col_blocks
    to2 = lax.dynamic_slice_in_dim(cols2, d * stored2, stored2, 0) - r * row_blocks
    mine = sparse_partial(keep, w1, to1, col_blocks, False)
    theirs = sparse_partial(taken, w1, to1, col_blocks, False)
    half = col_blocks // 2
    sent = jnp.stack([
        lax.dynamic_slice_in_dim(theirs, other * half, half, 0),
        lax.dynamic_slice_in_dim(mine, other * half, half, 0),
    ])
    held = jnp.stack([
        lax.dynamic_slice_in_dim(mine, d * half, half, 0),
        lax.dynamic_slice_in_dim(theirs, d * half, half, 0),
    ])
    came = lax.ppermute(sent.astype(bf16), "depth", swap)
    both = (held + came.astype(f32)).astype(bf16)
    share = half // n_row
    spread = lax.all_to_all(both.reshape(2, n_row, share, rows, block), "row", 1, 1)
    z1 = spread.astype(f32).sum(1)
    first = d * half + r * share
    bias_part = lax.dynamic_slice_in_dim(bias1.reshape(col_blocks, block), first, share, 0)
    live = jnp.stack([mask2, lax.ppermute(mask2.astype(f32), "depth", swap).astype(jnp.int32)])
    live = lax.dynamic_slice_in_dim(live, first, share, 2).transpose(0, 2, 1)
    x1 = (jnp.maximum(z1 + bias_part[:, None, :], 0.0) * live[..., None].astype(f32)).astype(bf16)
    x1 = lax.all_gather(x1, "row", axis=1, tiled=True)
    away = sparse_partial(x1[1], w2, to2, row_blocks, True, bf16)
    back = lax.ppermute(away, "depth", swap)
    home = sparse_partial(x1[0], w2, to2, row_blocks, True)
    z2 = (home + back.astype(f32)).astype(bf16)
    out_share = row_blocks // n_col
    z2 = lax.all_to_all(z2.reshape(n_col, out_share, rows, block), "col", 0, 0)
    z2 = z2.astype(f32).sum(0)
    out = jnp.maximum(z2 + bias2.reshape(out_share, 1, block), 0.0).astype(bf16)
    return out.transpose(1, 0, 2).reshape(rows, -1)


def solution(mesh):
    return jax.shard_map(
        exchanged_rows if mesh.shape["depth"] == 2 else gathered_weights,
        mesh=mesh,
        in_specs=(
            P("depth", "row"),
            P("depth", "row"),
            P(("row", "depth"), "col", None, None),
            P("row", "col"),
            P("col"),
            P("depth", "col"),
            P(("col", "depth"), "row", None, None),
            P("col", "row"),
            P(("row", "col")),
        ),
        out_specs=P("depth", ("row", "col")),
        check_vma=False,
    )
```

```python
import functools

import jax
import jax.numpy as jnp
from jax import lax
from jax.experimental import pallas as pl
from jax.experimental.pallas import tpu as pltpu
from jax.sharding import PartitionSpec as P


def fold_function(inputs, targets, stride):

    def add_tiles(running_total, tiles, first_row):

        def advance(number, total):
            offset = number * stride
            block_list = lax.dynamic_slice_in_dim(tiles, offset, stride, 0)
            incoming_rows = lax.dynamic_slice_in_dim(inputs, offset, stride, 1)
            wanted = lax.dynamic_slice_in_dim(targets, offset, stride, 0)
            product = jnp.einsum(
                "tws,wish->twih", incoming_rows, block_list, preferred_element_type=jnp.float32
            )
            flat_product = product.reshape(product.shape[0], -1, product.shape[-1])
            return total.at[:, wanted.reshape(-1)].add(flat_product)

        return lax.fori_loop(0, tiles.shape[0] // stride, advance, running_total)

    return add_tiles


def gathered_weights(acts, act_mask, w1, cols1, bias1, mask2, w2, cols2, bias2):
    block = w1.shape[-1]
    rows_dev = acts.shape[0]
    row_blocks = act_mask.shape[1]
    col_blocks = mask2.shape[1]
    row_index = lax.axis_index("row")
    col_index = lax.axis_index("col")
    masked = acts.reshape(rows_dev, row_blocks, block) * act_mask[:, :, None].astype(jnp.bfloat16)
    first_layer_destinations = cols1 - col_index * col_blocks
    second_targets = cols2 - row_index * row_blocks
    first_offset_value = jnp.zeros((rows_dev, col_blocks, block), jnp.float32)
    first_fold = fold_function(masked, first_layer_destinations, w1.shape[0])
    first_sum = first_fold(
        first_offset_value, lax.all_gather(w1, "depth", axis=0, tiled=True), jnp.int32(0)
    )
    bias_blocks = bias1.reshape(col_blocks, block)
    share = col_blocks // lax.axis_size("row")
    part_sum = lax.psum_scatter(first_sum, "row", scatter_dimension=1, tiled=True)
    bias_part = lax.dynamic_slice_in_dim(bias_blocks, row_index * share, share, 0)
    mask_part = lax.dynamic_slice_in_dim(mask2, row_index * share, share, 1)
    hidden_part = jnp.maximum(part_sum + bias_part, 0.0) * mask_part[:, :, None].astype(jnp.float32)
    hidden = lax.all_gather(hidden_part.astype(jnp.bfloat16), "row", axis=1, tiled=True)
    second_start = jnp.zeros((rows_dev, row_blocks, block), jnp.float32)
    second_fold = fold_function(hidden, second_targets, w2.shape[0])
    second_sum = second_fold(
        second_start, lax.all_gather(w2, "depth", axis=0, tiled=True), jnp.int32(0)
    )
    outcome = lax.psum_scatter(second_sum, "col", scatter_dimension=1, tiled=True)
    bias_out = bias2.reshape(outcome.shape[1], block)
    return jnp.maximum(outcome + bias_out, 0.0).astype(jnp.bfloat16).reshape(rows_dev, -1)


def sparse_kernel(per_step, entries, blocked, cols_ref, core_ref, x_ref, w_ref, *refs):
    *outs, total = refs
    step = pl.program_id(0)
    block = w_ref.shape[-1]

    @pl.when(step == 0)
    def _():
        total[...] = jnp.zeros_like(total)

    for row in range(per_step):
        if blocked:
            x = x_ref[row]
        else:
            x = x_ref[:, row * block:(row + 1) * block]
        for entry in range(0, entries, 2):
            pair = jnp.concatenate([w_ref[row, entry], w_ref[row, entry + 1]], axis=1)
            product = jnp.dot(x, pair, preferred_element_type=jnp.float32)
            base = (step * per_step + row) * entries + entry
            total[cols_ref[base]] += product[:, :block]
            total[cols_ref[base + 1]] += product[:, block:]

    @pl.when(step == pl.num_programs(0) - 1)
    def _():
        if len(outs) == 1:
            outs[0][...] = total[...].astype(outs[0].dtype)
        else:
            kept, given = outs
            pieces, size = kept.shape[:2]
            core = core_ref[0]
            for piece in range(pieces):
                start = piece * 2 * size
                kept[piece] = total[pl.ds(start + core * size, size)]
                given[piece] = total[pl.ds(start + (1 - core) * size, size)].astype(given.dtype)


def sparse_partial(x, weights, cols, core, out_blocks, blocked, outs):
    stored, entries, block, _ = weights.shape
    rows = x.shape[1] if blocked else x.shape[0]
    per_step = 4 if stored % 4 == 0 else 1
    if blocked:
        x_spec = pl.BlockSpec((per_step, rows, block), lambda i, *_: (i, 0, 0))
    else:
        x_spec = pl.BlockSpec((rows, per_step * block), lambda i, *_: (0, i))
    zeros = [(lambda n: lambda i, *_: (0,) * n)(len(out.shape)) for out in outs]
    return pl.pallas_call(
        functools.partial(sparse_kernel, per_step, entries, blocked),
        out_shape=outs,
        grid_spec=pltpu.PrefetchScalarGridSpec(
            num_scalar_prefetch=2,
            grid=(stored // per_step,),
            in_specs=[
                x_spec,
                pl.BlockSpec((per_step, entries, block, block), lambda i, *_: (i, 0, 0, 0)),
            ],
            out_specs=[pl.BlockSpec(out.shape, zero) for out, zero in zip(outs, zeros)],
            scratch_shapes=[pltpu.VMEM((out_blocks, rows, block), jnp.float32)],
        ),
        compiler_params=pltpu.CompilerParams(
            dimension_semantics=("arbitrary",), vmem_limit_bytes=40 * 1024 * 1024
        ),
        cost_estimate=pl.CostEstimate(
            flops=2 * rows * weights.size, bytes_accessed=2 * weights.size, transcendentals=0
        ),
    )(cols.reshape(-1), core.reshape(1), x, weights)


MESH = pl.DeviceIdType.MESH
F32, BF16 = jnp.float32, jnp.bfloat16


def greet(partners):
    barrier = pltpu.get_barrier_semaphore()
    for partner in partners:
        pl.semaphore_signal(barrier, inc=1, device_id=partner, device_id_type=MESH)
    pl.semaphore_wait(barrier, len(partners))


def first_reduce_kernel(
    chunks, kept0, kept1, given0, given1, bias, live, out,
    core_in, total, y_out, y_in, x_out, x_in, send_sem, recv_sem,
):
    r, d = lax.axis_index("row"), lax.axis_index("depth")
    x, core = r // 2, r % 2
    partner = {"row": x * 2 + 1 - core}
    y_peer = {"depth": 1 - d}
    x_peer = {"row": (1 - x) * 2 + core}
    kept, given = (kept0, kept1), (given0, given1)
    size = kept0.shape[2] // chunks
    steps = [(half, part) for part in range(chunks) for half in range(2)]
    arrivals = [(1 - half, part) for half, part in steps]
    started = []

    def send(stage, source, target, step, landing, device):
        copy = pltpu.make_async_remote_copy(
            src_ref=source, dst_ref=target,
            send_sem=send_sem.at[stage, step[0], step[1]],
            recv_sem=recv_sem.at[stage, landing[0], landing[1]],
            device_id=device, device_id_type=MESH,
        )
        copy.start()
        started.append(copy)

    def await_arrival(stage, target, step):
        pltpu.make_async_remote_copy(
            src_ref=target, dst_ref=target,
            send_sem=send_sem.at[stage, step[0], step[1]],
            recv_sem=recv_sem.at[stage, step[0], step[1]],
            device_id=x_peer, device_id_type=MESH,
        ).wait_recv()

    greet([partner, y_peer, x_peer])
    for step in steps:
        half, part = step
        cut = pl.ds(part * size, size)
        send(0, given[half].at[:, :, cut], core_in.at[half, part], step, step, partner)

    def pair(step):
        half, part = step
        cut = pl.ds(part * size, size)
        await_arrival(0, core_in.at[half, part], step)
        y_out[half, part] = (
            kept[half][1 - d, :, cut] + core_in[half, part, 1 - d].astype(F32)
        ).astype(BF16)
        send(1, y_out.at[half, part], y_in.at[1 - half, part], step, (1 - half, part), y_peer)
        total[half, part] = kept[half][d, :, cut] + core_in[half, part, d].astype(F32)

    def along_y(step):
        half, part = step
        await_arrival(1, y_in.at[half, part], step)
        x_out[half, part] = (
            total[half, part, 1 - x] + y_in[half, part, 1 - x].astype(F32)
        ).astype(BF16)
        send(2, x_out.at[half, part], x_in.at[half, part], step, step, x_peer)

    def along_x(step):
        half, part = step
        cut = pl.ds(part * size, size)
        await_arrival(2, x_in.at[half, part], step)
        z = total[half, part, x] + y_in[half, part, x].astype(F32) + x_in[half, part].astype(F32)
        for b in range(size):
            at = part * size + b
            value = jnp.maximum(z[b] + bias[at:at + 1, :], 0.0) * live[half, :, at:at + 1]
            out[half, x, core, at] = value.astype(BF16)
        mine = out.at[half, x, core, cut]
        send(3, mine, mine, step, step, x_peer)
        send(4, mine, mine, step, step, partner)

    def forward(step):
        half, part = step
        cut = pl.ds(part * size, size)
        await_arrival(3, out.at[half, 1 - x, core, cut], step)
        theirs = out.at[half, 1 - x, core, cut]
        send(5, theirs, theirs, step, step, partner)

    count = len(steps)
    for at in range(count + 3):
        if at < count:
            pair(steps[at])
        if 0 <= at - 1 < count:
            along_y(arrivals[at - 1])
        if 0 <= at - 2 < count:
            along_x(arrivals[at - 2])
        if 0 <= at - 3 < count:
            forward(arrivals[at - 3])
    for step in arrivals:
        half, part = step
        cut = pl.ds(part * size, size)
        await_arrival(4, out.at[half, x, 1 - core, cut], step)
        await_arrival(5, out.at[half, 1 - x, 1 - core, cut], step)
    for copy in started:
        copy.wait_send()


def first_reduce(kept, given, bias, live):
    _, _, share, rows, block = kept[0].shape
    chunks = 2 if share % 2 == 0 else 1
    size = share // chunks
    vmem = pl.BlockSpec(memory_space=pltpu.VMEM)
    return pl.pallas_call(
        functools.partial(first_reduce_kernel, chunks),
        out_shape=jax.ShapeDtypeStruct((2, 2, 2, share, rows, block), BF16),
        in_specs=[vmem] * 6,
        out_specs=vmem,
        scratch_shapes=[
            pltpu.VMEM((2, chunks, 2, 2, size, rows, block), BF16),
            pltpu.VMEM((2, chunks, 2, size, rows, block), F32),
            pltpu.VMEM((2, chunks, 2, size, rows, block), BF16),
            pltpu.VMEM((2, chunks, 2, size, rows, block), BF16),
            pltpu.VMEM((2, chunks, size, rows, block), BF16),
            pltpu.VMEM((2, chunks, size, rows, block), BF16),
            pltpu.SemaphoreType.DMA((6, 2, chunks)),
            pltpu.SemaphoreType.DMA((6, 2, chunks)),
        ],
        compiler_params=pltpu.CompilerParams(
            collective_id=1, has_side_effects=True, vmem_limit_bytes=48 * 1024 * 1024
        ),
        name="first_reduce",
    )(*kept, *given, bias, live)


def second_reduce_kernel(n_col, parts, home, away, bias, out, y_in, z_out, z_in, send_y, recv_y, send_z, recv_z):
    c, d = lax.axis_index("col"), lax.axis_index("depth")
    share, block = out.shape[1] // home.shape[2], home.shape[2]
    size = home.shape[1] // parts
    y_peer = {"depth": 1 - d}
    offsets = sorted(range(1, n_col), key=lambda o: -min(o, n_col - o)) + [0]
    steps = [(o, p) for o in offsets for p in range(parts)]

    def target(o):
        return lax.rem(c + o, n_col)

    def y_copy(o, p):
        return pltpu.make_async_remote_copy(
            src_ref=away.at[pl.ds(target(o) * share, share), pl.ds(p * size, size)],
            dst_ref=y_in.at[o, p],
            send_sem=send_y.at[o, p], recv_sem=recv_y.at[o, p],
            device_id=y_peer, device_id_type=MESH,
        )

    def z_copy(o, p):
        return pltpu.make_async_remote_copy(
            src_ref=z_out.at[o - 1, p], dst_ref=z_in.at[o - 1, p],
            send_sem=send_z.at[o - 1, p], recv_sem=recv_z.at[o - 1, p],
            device_id={"col": target(o)}, device_id_type=MESH,
        )

    greet([y_peer] + [{"col": target(o)} for o in range(1, n_col)])
    for o, p in steps:
        y_copy(o, p).start()
    for o, p in steps:
        if o == 0:
            continue
        y_copy(o, p).wait_recv()
        z_out[o - 1, p] = (
            home[pl.ds(target(o) * share, share), p * size:(p + 1) * size]
            + y_in[o, p].astype(F32)
        ).astype(BF16)
        z_copy(o, p).start()
    for p in range(parts):
        y_copy(0, p).wait_recv()
        for o in range(1, n_col):
            z_copy(o, p).wait_recv()
        for b in range(share):
            value = home[c * share + b, p * size:(p + 1) * size] + y_in[0, p, b].astype(F32)
            for o in range(1, n_col):
                value += z_in[o - 1, p, b].astype(F32)
            value = jnp.maximum(value + bias[b:b + 1, :], 0.0)
            out[p * size:(p + 1) * size, b * block:(b + 1) * block] = value.astype(BF16)
    for o, p in steps:
        y_copy(o, p).wait_send()
        if o:
            z_copy(o, p).wait_send()


def second_reduce(home, away, bias, n_col):
    blocks, rows, block = home.shape
    share = blocks // n_col
    parts = 2
    size = rows // parts
    vmem = pl.BlockSpec(memory_space=pltpu.VMEM)
    return pl.pallas_call(
        functools.partial(second_reduce_kernel, n_col, parts),
        out_shape=jax.ShapeDtypeStruct((rows, share * block), BF16),
        in_specs=[vmem] * 3,
        out_specs=vmem,
        scratch_shapes=[
            pltpu.VMEM((n_col, parts, share, size, block), BF16),
            pltpu.VMEM((n_col - 1, parts, share, size, block), BF16),
            pltpu.VMEM((n_col - 1, parts, share, size, block), BF16),
            pltpu.SemaphoreType.DMA((n_col, parts)),
            pltpu.SemaphoreType.DMA((n_col, parts)),
            pltpu.SemaphoreType.DMA((n_col - 1, parts)),
            pltpu.SemaphoreType.DMA((n_col - 1, parts)),
        ],
        compiler_params=pltpu.CompilerParams(
            collective_id=2, has_side_effects=True, vmem_limit_bytes=48 * 1024 * 1024
        ),
        name="second_reduce",
    )(home, away, bias)


def exchanged_rows(acts, act_mask, w1, cols1, bias1, mask2, w2, cols2, bias2):
    block = w1.shape[-1]
    stored1, stored2 = w1.shape[0], w2.shape[0]
    rows = acts.shape[0]
    row_blocks, col_blocks = act_mask.shape[1], mask2.shape[1]
    r, c, d = lax.axis_index("row"), lax.axis_index("col"), lax.axis_index("depth")
    n_row, n_col = lax.axis_size("row"), lax.axis_size("col")
    other = 1 - d
    swap = [(0, 1), (1, 0)]
    masked = (acts.reshape(rows, row_blocks, block) * act_mask[:, :, None].astype(BF16)).reshape(rows, -1)
    keep = lax.dynamic_slice_in_dim(masked, d * stored1 * block, stored1 * block, 1)
    give = lax.dynamic_slice_in_dim(masked, other * stored1 * block, stored1 * block, 1)
    taken = lax.ppermute(give, "depth", swap)
    to1 = lax.dynamic_slice_in_dim(cols1, d * stored1, stored1, 0) - c * col_blocks
    to2 = lax.dynamic_slice_in_dim(cols2, d * stored2, stored2, 0) - r * row_blocks
    core = r % 2
    share = col_blocks // 2 // n_row
    shape1 = (col_blocks // share // 2, share, rows, block)
    outs1 = [jax.ShapeDtypeStruct(shape1, F32), jax.ShapeDtypeStruct(shape1, BF16)]
    kept0, given0 = sparse_partial(keep, w1, to1, core, col_blocks, False, outs1)
    kept1, given1 = sparse_partial(taken, w1, to1, core, col_blocks, False, outs1)
    first = d * (col_blocks // 2) + r * share
    bias_part = lax.dynamic_slice_in_dim(bias1.reshape(col_blocks, block), first, share, 0)
    live = jnp.stack([mask2.astype(F32), lax.ppermute(mask2.astype(F32), "depth", swap)])
    live = lax.dynamic_slice_in_dim(live, first, share, 2)
    split = (2, n_row // 2, share, rows, block)
    x1 = first_reduce(
        [kept0.reshape(split), kept1.reshape(split)],
        [given0.reshape(split), given1.reshape(split)],
        bias_part, live,
    ).reshape(2, col_blocks // 2, rows, block)
    shape2 = (row_blocks, rows, block)
    (away,) = sparse_partial(x1[1], w2, to2, core, row_blocks, True, [jax.ShapeDtypeStruct(shape2, BF16)])
    (home,) = sparse_partial(x1[0], w2, to2, core, row_blocks, True, [jax.ShapeDtypeStruct(shape2, F32)])
    return second_reduce(home, away, bias2.reshape(row_blocks // n_col, block), n_col)


def solution(mesh):
    near = mesh.shape["depth"] == 2 and mesh.shape["row"] == 4
    return jax.shard_map(
        exchanged_rows if near else gathered_weights,
        mesh=mesh,
        in_specs=(
            P("depth", "row"),
            P("depth", "row"),
            P(("row", "depth"), "col", None, None),
            P("row", "col"),
            P("col"),
            P("depth", "col"),
            P(("col", "depth"), "row", None, None),
            P("col", "row"),
            P(("row", "col")),
        ),
        out_specs=P("depth", ("row", "col")),
        check_vma=False,
    )
```

```python
import functools

import jax
import jax.numpy as jnp
from jax import lax
from jax.experimental import pallas as pl
from jax.experimental.pallas import tpu as pltpu
from jax.sharding import PartitionSpec as P


def fold_function(inputs, targets, stride):

    def add_tiles(running_total, tiles, first_row):

        def advance(number, total):
            offset = number * stride
            block_list = lax.dynamic_slice_in_dim(tiles, offset, stride, 0)
            incoming_rows = lax.dynamic_slice_in_dim(inputs, offset, stride, 1)
            wanted = lax.dynamic_slice_in_dim(targets, offset, stride, 0)
            product = jnp.einsum(
                "tws,wish->twih", incoming_rows, block_list, preferred_element_type=jnp.float32
            )
            flat_product = product.reshape(product.shape[0], -1, product.shape[-1])
            return total.at[:, wanted.reshape(-1)].add(flat_product)

        return lax.fori_loop(0, tiles.shape[0] // stride, advance, running_total)

    return add_tiles


def gathered_weights(acts, act_mask, w1, cols1, bias1, mask2, w2, cols2, bias2):
    block = w1.shape[-1]
    rows_dev = acts.shape[0]
    row_blocks = act_mask.shape[1]
    col_blocks = mask2.shape[1]
    row_index = lax.axis_index("row")
    col_index = lax.axis_index("col")
    masked = acts.reshape(rows_dev, row_blocks, block) * act_mask[:, :, None].astype(jnp.bfloat16)
    first_layer_destinations = cols1 - col_index * col_blocks
    second_targets = cols2 - row_index * row_blocks
    first_offset_value = jnp.zeros((rows_dev, col_blocks, block), jnp.float32)
    first_fold = fold_function(masked, first_layer_destinations, w1.shape[0])
    first_sum = first_fold(
        first_offset_value, lax.all_gather(w1, "depth", axis=0, tiled=True), jnp.int32(0)
    )
    bias_blocks = bias1.reshape(col_blocks, block)
    share = col_blocks // lax.axis_size("row")
    part_sum = lax.psum_scatter(first_sum, "row", scatter_dimension=1, tiled=True)
    bias_part = lax.dynamic_slice_in_dim(bias_blocks, row_index * share, share, 0)
    mask_part = lax.dynamic_slice_in_dim(mask2, row_index * share, share, 1)
    hidden_part = jnp.maximum(part_sum + bias_part, 0.0) * mask_part[:, :, None].astype(jnp.float32)
    hidden = lax.all_gather(hidden_part.astype(jnp.bfloat16), "row", axis=1, tiled=True)
    second_start = jnp.zeros((rows_dev, row_blocks, block), jnp.float32)
    second_fold = fold_function(hidden, second_targets, w2.shape[0])
    second_sum = second_fold(
        second_start, lax.all_gather(w2, "depth", axis=0, tiled=True), jnp.int32(0)
    )
    outcome = lax.psum_scatter(second_sum, "col", scatter_dimension=1, tiled=True)
    bias_out = bias2.reshape(outcome.shape[1], block)
    return jnp.maximum(outcome + bias_out, 0.0).astype(jnp.bfloat16).reshape(rows_dev, -1)


def sparse_kernel(per_step, entries, blocked, cols_ref, core_ref, x_ref, w_ref, *refs):
    *outs, total = refs
    step = pl.program_id(0)
    block = w_ref.shape[-1]

    @pl.when(step == 0)
    def _():
        total[...] = jnp.zeros_like(total)

    for row in range(per_step):
        if blocked:
            x = x_ref[:, row].reshape(-1, block)
        else:
            x = x_ref[:, row * block:(row + 1) * block]
        for entry in range(0, entries, 2):
            pair = jnp.concatenate([w_ref[row, entry], w_ref[row, entry + 1]], axis=1)
            product = jnp.dot(x, pair, preferred_element_type=jnp.float32)
            base = (step * per_step + row) * entries + entry
            total[cols_ref[base]] += product[:, :block]
            total[cols_ref[base + 1]] += product[:, block:]

    @pl.when(step == pl.num_programs(0) - 1)
    def _():
        if blocked:
            rows = outs[0].shape[1]
            for half, out in enumerate(outs):
                out[...] = total[:, half * rows:(half + 1) * rows].astype(out.dtype)
        else:
            kept, given = outs
            pieces, size = kept.shape[:2]
            core = core_ref[0]
            for piece in range(pieces):
                start = piece * 2 * size
                kept[piece] = total[pl.ds(start + core * size, size)]
                given[piece] = total[pl.ds(start + (1 - core) * size, size)].astype(given.dtype)


def sparse_partial(x, weights, cols, core, out_blocks, blocked, outs):
    stored, entries, block, _ = weights.shape
    rows = x.shape[2] if blocked else x.shape[0]
    lines = 2 * rows if blocked else rows
    per_step = 4 if stored % 4 == 0 else 1
    if blocked:
        x_spec = pl.BlockSpec((2, per_step, rows, block), lambda i, *_: (0, i, 0, 0))
    else:
        x_spec = pl.BlockSpec((rows, per_step * block), lambda i, *_: (0, i))
    zeros = [(lambda n: lambda i, *_: (0,) * n)(len(out.shape)) for out in outs]
    return pl.pallas_call(
        functools.partial(sparse_kernel, per_step, entries, blocked),
        out_shape=outs,
        grid_spec=pltpu.PrefetchScalarGridSpec(
            num_scalar_prefetch=2,
            grid=(stored // per_step,),
            in_specs=[
                x_spec,
                pl.BlockSpec((per_step, entries, block, block), lambda i, *_: (i, 0, 0, 0)),
            ],
            out_specs=[pl.BlockSpec(out.shape, zero) for out, zero in zip(outs, zeros)],
            scratch_shapes=[pltpu.VMEM((out_blocks, lines, block), jnp.float32)],
        ),
        compiler_params=pltpu.CompilerParams(
            dimension_semantics=("arbitrary",), vmem_limit_bytes=40 * 1024 * 1024
        ),
        cost_estimate=pl.CostEstimate(
            flops=2 * lines * weights.size, bytes_accessed=2 * weights.size, transcendentals=0
        ),
    )(cols.reshape(-1), core.reshape(1), x, weights)


MESH = pl.DeviceIdType.MESH
F32, BF16 = jnp.float32, jnp.bfloat16


def greet(partners):
    barrier = pltpu.get_barrier_semaphore()
    for partner in partners:
        pl.semaphore_signal(barrier, inc=1, device_id=partner, device_id_type=MESH)
    pl.semaphore_wait(barrier, len(partners))


def first_reduce_kernel(
    chunks, kept0, kept1, given0, given1, bias, live, out,
    core_in, total, y_out, y_in, x_out, x_in, send_sem, recv_sem,
):
    r, d = lax.axis_index("row"), lax.axis_index("depth")
    x, core = r // 2, r % 2
    partner = {"row": x * 2 + 1 - core}
    y_peer = {"depth": 1 - d}
    x_peer = {"row": (1 - x) * 2 + core}
    kept, given = (kept0, kept1), (given0, given1)
    size = kept0.shape[2] // chunks
    steps = [(half, part) for part in range(chunks) for half in range(2)]
    arrivals = [(1 - half, part) for half, part in steps]
    started = []

    def send(stage, source, target, step, landing, device):
        copy = pltpu.make_async_remote_copy(
            src_ref=source, dst_ref=target,
            send_sem=send_sem.at[stage, step[0], step[1]],
            recv_sem=recv_sem.at[stage, landing[0], landing[1]],
            device_id=device, device_id_type=MESH,
        )
        copy.start()
        started.append(copy)

    def await_arrival(stage, target, step):
        pltpu.make_async_remote_copy(
            src_ref=target, dst_ref=target,
            send_sem=send_sem.at[stage, step[0], step[1]],
            recv_sem=recv_sem.at[stage, step[0], step[1]],
            device_id=x_peer, device_id_type=MESH,
        ).wait_recv()

    greet([partner, y_peer, x_peer])
    for step in steps:
        half, part = step
        cut = pl.ds(part * size, size)
        send(0, given[half].at[:, :, cut], core_in.at[half, part], step, step, partner)

    def pair(step):
        half, part = step
        cut = pl.ds(part * size, size)
        await_arrival(0, core_in.at[half, part], step)
        y_out[half, part] = (
            kept[half][1 - d, :, cut] + core_in[half, part, 1 - d].astype(F32)
        ).astype(BF16)
        send(1, y_out.at[half, part], y_in.at[1 - half, part], step, (1 - half, part), y_peer)
        total[half, part] = kept[half][d, :, cut] + core_in[half, part, d].astype(F32)

    def along_y(step):
        half, part = step
        await_arrival(1, y_in.at[half, part], step)
        x_out[half, part] = (
            total[half, part, 1 - x] + y_in[half, part, 1 - x].astype(F32)
        ).astype(BF16)
        send(2, x_out.at[half, part], x_in.at[half, part], step, step, x_peer)

    def along_x(step):
        half, part = step
        cut = pl.ds(part * size, size)
        await_arrival(2, x_in.at[half, part], step)
        z = total[half, part, x] + y_in[half, part, x].astype(F32) + x_in[half, part].astype(F32)
        for b in range(size):
            at = part * size + b
            value = jnp.maximum(z[b] + bias[at:at + 1, :], 0.0) * live[half, :, at:at + 1]
            out[half, x, core, at] = value.astype(BF16)
        mine = out.at[half, x, core, cut]
        send(3, mine, mine, step, step, x_peer)
        send(4, mine, mine, step, step, partner)

    def forward(step):
        half, part = step
        cut = pl.ds(part * size, size)
        await_arrival(3, out.at[half, 1 - x, core, cut], step)
        theirs = out.at[half, 1 - x, core, cut]
        send(5, theirs, theirs, step, step, partner)

    count = len(steps)
    for at in range(count + 3):
        if at < count:
            pair(steps[at])
        if 0 <= at - 1 < count:
            along_y(arrivals[at - 1])
        if 0 <= at - 2 < count:
            along_x(arrivals[at - 2])
        if 0 <= at - 3 < count:
            forward(arrivals[at - 3])
    for step in arrivals:
        half, part = step
        cut = pl.ds(part * size, size)
        await_arrival(4, out.at[half, x, 1 - core, cut], step)
        await_arrival(5, out.at[half, 1 - x, 1 - core, cut], step)
    for copy in started:
        copy.wait_send()


def first_reduce(kept, given, bias, live):
    _, _, share, rows, block = kept[0].shape
    chunks = 4 if share % 4 == 0 else 1
    size = share // chunks
    vmem = pl.BlockSpec(memory_space=pltpu.VMEM)
    return pl.pallas_call(
        functools.partial(first_reduce_kernel, chunks),
        out_shape=jax.ShapeDtypeStruct((2, 2, 2, share, rows, block), BF16),
        in_specs=[vmem] * 6,
        out_specs=vmem,
        scratch_shapes=[
            pltpu.VMEM((2, chunks, 2, 2, size, rows, block), BF16),
            pltpu.VMEM((2, chunks, 2, size, rows, block), F32),
            pltpu.VMEM((2, chunks, 2, size, rows, block), BF16),
            pltpu.VMEM((2, chunks, 2, size, rows, block), BF16),
            pltpu.VMEM((2, chunks, size, rows, block), BF16),
            pltpu.VMEM((2, chunks, size, rows, block), BF16),
            pltpu.SemaphoreType.DMA((6, 2, chunks)),
            pltpu.SemaphoreType.DMA((6, 2, chunks)),
        ],
        compiler_params=pltpu.CompilerParams(
            collective_id=1, has_side_effects=True, vmem_limit_bytes=48 * 1024 * 1024
        ),
        name="first_reduce",
    )(*kept, *given, bias, live)


def second_reduce_kernel(n_col, parts, home, away, bias, out, y_in, z_out, z_in, send_y, recv_y, send_z, recv_z):
    c, d = lax.axis_index("col"), lax.axis_index("depth")
    share, block = out.shape[1] // home.shape[2], home.shape[2]
    size = home.shape[1] // parts
    last = n_col - 1
    upper = c // 2
    inner = c + upper * (last - 2 * c)
    y_peer = {"depth": 1 - d}
    steps = [(i, p) for i in range(n_col) for p in range(parts)]

    def mirrored(value):
        return value + upper * (last - 2 * value)

    def owner(i):
        end, mid = (3, 2, 1, 0)[i], (2, 0, 3, 1)[i]
        return mirrored(end + inner * (mid - end))

    def receiver(i):
        end, mid = (1, 2, 1)[i], (2, 0, 3)[i]
        return mirrored(end + inner * (mid - end))

    def y_copy(i, p):
        return pltpu.make_async_remote_copy(
            src_ref=away.at[pl.ds(owner(i) * share, share), pl.ds(p * size, size)],
            dst_ref=y_in.at[i, p],
            send_sem=send_y.at[i, p], recv_sem=recv_y.at[i, p],
            device_id=y_peer, device_id_type=MESH,
        )

    def z_copy(i, p):
        slot = 3 * inner if i == 0 else i
        return pltpu.make_async_remote_copy(
            src_ref=z_out.at[i, p], dst_ref=z_in.at[slot, p],
            send_sem=send_z.at[i, p], recv_sem=recv_z.at[slot, p],
            device_id={"col": receiver(i)}, device_id_type=MESH,
        )

    def z_arrival(slot, p):
        pltpu.make_async_remote_copy(
            src_ref=z_in.at[slot, p], dst_ref=z_in.at[slot, p],
            send_sem=send_z.at[0, p], recv_sem=recv_z.at[slot, p],
            device_id={"col": receiver(0)}, device_id_type=MESH,
        ).wait_recv()

    greet([y_peer] + [{"col": lax.rem(c + o, n_col)} for o in range(1, n_col)])
    for i, p in steps:
        y_copy(i, p).start()

    def near_sum(i, p):
        return home[pl.ds(owner(i) * share, share), p * size:(p + 1) * size] + y_in[i, p].astype(F32)

    for i, p in steps[:-parts]:
        y_copy(i, p).wait_recv()
        if i == 2:
            @pl.when(inner == 1)
            def _():
                z_arrival(0, p)
                z_out[i, p] = (near_sum(i, p) + z_in[0, p].astype(F32)).astype(BF16)

            @pl.when(inner == 0)
            def _():
                z_out[i, p] = near_sum(i, p).astype(BF16)
        else:
            z_out[i, p] = near_sum(i, p).astype(BF16)
        z_copy(i, p).start()

    def finish(p, slots):
        for slot in slots:
            z_arrival(slot, p)
        for b in range(share):
            value = home[c * share + b, p * size:(p + 1) * size] + y_in[n_col - 1, p, b].astype(F32)
            for slot in slots:
                value += z_in[slot, p, b].astype(F32)
            value = jnp.maximum(value + bias[b:b + 1, :], 0.0)
            out[p * size:(p + 1) * size, b * block:(b + 1) * block] = value.astype(BF16)

    for p in range(parts):
        y_copy(n_col - 1, p).wait_recv()

        @pl.when(inner == 1)
        def _():
            finish(p, (1, 2, 3))

        @pl.when(inner == 0)
        def _():
            finish(p, (1, 2))
    for i, p in steps:
        y_copy(i, p).wait_send()
        if i < n_col - 1:
            z_copy(i, p).wait_send()


def second_reduce(home, away, bias, n_col):
    blocks, rows, block = home.shape
    share = blocks // n_col
    parts = 2
    size = rows // parts
    vmem = pl.BlockSpec(memory_space=pltpu.VMEM)
    return pl.pallas_call(
        functools.partial(second_reduce_kernel, n_col, parts),
        out_shape=jax.ShapeDtypeStruct((rows, share * block), BF16),
        in_specs=[vmem] * 3,
        out_specs=vmem,
        scratch_shapes=[
            pltpu.VMEM((n_col, parts, share, size, block), BF16),
            pltpu.VMEM((n_col - 1, parts, share, size, block), BF16),
            pltpu.VMEM((n_col, parts, share, size, block), BF16),
            pltpu.SemaphoreType.DMA((n_col, parts)),
            pltpu.SemaphoreType.DMA((n_col, parts)),
            pltpu.SemaphoreType.DMA((n_col - 1, parts)),
            pltpu.SemaphoreType.DMA((n_col, parts)),
        ],
        compiler_params=pltpu.CompilerParams(
            collective_id=2, has_side_effects=True, vmem_limit_bytes=48 * 1024 * 1024
        ),
        name="second_reduce",
    )(home, away, bias)


def exchanged_rows(acts, act_mask, w1, cols1, bias1, mask2, w2, cols2, bias2):
    block = w1.shape[-1]
    stored1, stored2 = w1.shape[0], w2.shape[0]
    rows = acts.shape[0]
    row_blocks, col_blocks = act_mask.shape[1], mask2.shape[1]
    r, c, d = lax.axis_index("row"), lax.axis_index("col"), lax.axis_index("depth")
    n_row, n_col = lax.axis_size("row"), lax.axis_size("col")
    other = 1 - d
    swap = [(0, 1), (1, 0)]
    masked = (acts.reshape(rows, row_blocks, block) * act_mask[:, :, None].astype(BF16)).reshape(rows, -1)
    keep = lax.dynamic_slice_in_dim(masked, d * stored1 * block, stored1 * block, 1)
    give = lax.dynamic_slice_in_dim(masked, other * stored1 * block, stored1 * block, 1)
    taken = lax.ppermute(give, "depth", swap)
    to1 = lax.dynamic_slice_in_dim(cols1, d * stored1, stored1, 0) - c * col_blocks
    to2 = lax.dynamic_slice_in_dim(cols2, d * stored2, stored2, 0) - r * row_blocks
    core = r % 2
    share = col_blocks // 2 // n_row
    shape1 = (col_blocks // share // 2, share, rows, block)
    outs1 = [jax.ShapeDtypeStruct(shape1, F32), jax.ShapeDtypeStruct(shape1, BF16)]
    kept0, given0 = sparse_partial(keep, w1, to1, core, col_blocks, False, outs1)
    kept1, given1 = sparse_partial(taken, w1, to1, core, col_blocks, False, outs1)
    first = d * (col_blocks // 2) + r * share
    bias_part = lax.dynamic_slice_in_dim(bias1.reshape(col_blocks, block), first, share, 0)
    live = jnp.stack([mask2.astype(F32), lax.ppermute(mask2.astype(F32), "depth", swap)])
    live = lax.dynamic_slice_in_dim(live, first, share, 2)
    split = (2, n_row // 2, share, rows, block)
    x1 = first_reduce(
        [kept0.reshape(split), kept1.reshape(split)],
        [given0.reshape(split), given1.reshape(split)],
        bias_part, live,
    ).reshape(2, col_blocks // 2, rows, block)
    shape2 = (row_blocks, rows, block)
    outs2 = [jax.ShapeDtypeStruct(shape2, F32), jax.ShapeDtypeStruct(shape2, BF16)]
    home, away = sparse_partial(x1, w2, to2, core, row_blocks, True, outs2)
    return second_reduce(home, away, bias2.reshape(row_blocks // n_col, block), n_col)


def solution(mesh):
    near = mesh.shape["depth"] == 2 and mesh.shape["row"] == 4 and mesh.shape["col"] == 4
    return jax.shard_map(
        exchanged_rows if near else gathered_weights,
        mesh=mesh,
        in_specs=(
            P("depth", "row"),
            P("depth", "row"),
            P(("row", "depth"), "col", None, None),
            P("row", "col"),
            P("col"),
            P("depth", "col"),
            P(("col", "depth"), "row", None, None),
            P("col", "row"),
            P(("row", "col")),
        ),
        out_specs=P("depth", ("row", "col")),
        check_vma=False,
    )
```
